256 devices in a mesh: pipe: 16 (over y, z_lo), tensor: 16 (over x, z_hi, core).
Axes of the slice: x: 4, y: 4, z: 8 (z_hi: 2, z_lo: 4; z = z_hi * 4 + z_lo), core: 2. Of those that a mesh axis runs over, the one named last changes fastest.
Arguments:
- memory: bfloat16 [2, 512, 4096], P(None, 'pipe', 'tensor'), may hold values from -6 to 6
- states: bfloat16 [16, 2, 256, 4096], P('pipe', None, None, 'tensor'), may hold values from -6 to 6
- norm_gain: float32 [16, 4096], P('pipe'), may hold values from 0.25 to 1.75
- w_query: bfloat16 [16, 4096, 4096], P('pipe', None, 'tensor'), may hold values from -0.09375 to 0.09375
- w_keyvalue: bfloat16 [16, 4096, 2, 4096], P('pipe', None, None, 'tensor'), may hold values from -0.09375 to 0.09375
- w_output: bfloat16 [16, 4096, 4096], P('pipe', 'tensor'), may hold values from -0.125 to 0.125
Outputs:
- updated: bfloat16 [16, 2, 256, 4096], P('pipe', None, None, 'tensor')
The draws below stay inside these ranges and needn't reach their ends.
All inputs are finite; a program needn't handle non-finite values.
Results may differ from the reference program's by a relative error of at most 0.006.
Values may be sent and summed in bfloat16 or wider, within the bound.
No kernel may reach another device: no remote copies, remote signals or barrier semaphores. Data moves between devices by JAX's collectives and lax.ppermute only.
A program may use at most 128 MiB of HBM per device.

```python
import jax
import jax.numpy as jnp
from jax import lax

D = 4096
HEADS = 64
HEAD_DIM = 64
INNER = 4096
SEQS = 2
ENC_LEN = 512
DEC_LEN = 256
SECTIONS = 16


def with_spikes(entries, stream_key, source, target, parts, factor):
    owner, partner = [(jnp.arange(entries.shape[dim]) // (entries.shape[dim] // parts)).reshape([-1 if axis == dim else 1 for axis in range(entries.ndim)]) for dim in (source, target)]
    chosen = jax.random.permutation(stream_key, parts)[partner]
    strong = (owner == chosen) | (owner == (partner + parts // 2) % parts)
    return jnp.where(strong, factor * entries, entries)


def levels(own_key, extent, shards, low, largest):
    level, own = 1.0, jax.random.fold_in(own_key, 6)
    for dim, parts in shards:
        steps = jnp.exp(jax.random.uniform(jax.random.fold_in(own, dim), (parts,), jnp.float32, low / len(shards), largest / len(shards)))
        level = level * jnp.repeat(steps, extent[dim] // parts).reshape([-1 if axis == dim else 1 for axis in range(len(extent))])
    return level


def scatter_about(rng, extent, scale, reach, split=(), held_as=jnp.bfloat16):
    result = jax.random.normal(rng, extent, jnp.float32) * scale
    if len(split) > 0:
        result = levels(rng, extent, split, -0.22, 0.18) * result
    return jnp.clip(result, min=-reach, max=reach).astype(held_as)


def noise_with(own_key, shape, spread, reach, split, heavy, dtype=jnp.bfloat16):
    values = spread * jax.random.normal(own_key, shape, jnp.float32)
    if split:
        values = values * levels(own_key, shape, split, -0.22, 0.18)
    return jnp.clip(with_spikes(values, jax.random.fold_in(own_key, 3), *heavy), -reach, reach).astype(dtype)


def setup_inputs(seed: int = 0) -> dict:
    key_of = jax.random.split(jax.random.key(seed), 7)
    return {
        "memory": scatter_about(key_of[0], (SEQS, ENC_LEN, D), 1.0, 6.0, ((1, 16), (2, 16))),
        "states": scatter_about(key_of[1], (SECTIONS, SEQS, DEC_LEN, D), 1.0, 6.0, ((0, 16), (3, 16))),
        "norm_gain": jnp.clip(1.0 + 0.15 * jax.random.normal(key_of[2], (SECTIONS, D), jnp.float32), 0.25, 1.75),
        "w_query": scatter_about(key_of[3], (SECTIONS, D, INNER), D ** -0.5, 0.09375, ((0, 16), (2, 16))),
        "w_keyvalue": scatter_about(key_of[4], (SECTIONS, D, 2, INNER), D ** -0.5, 0.09375, ((0, 16), (3, 16))),
        "w_output": noise_with(key_of[5], (SECTIONS, INNER, D), INNER ** -0.5, 0.125, ((0, 16), (1, 16)), (1, 2, 16, 2.0)),
    }


def one_section(memory, section_states, gain, wq, wkv, wo):
    xf = section_states.astype(jnp.float32)
    scale = lax.rsqrt(lax.optimization_barrier(jnp.mean(xf * xf, axis=-1, keepdims=True)) + 1e-06)
    normed = (xf * scale * gain).astype(jnp.bfloat16)
    seqs = normed.shape[0]
    inner = HEADS * HEAD_DIM
    wkv_flat = wkv.reshape(wkv.shape[0], 2 * inner)
    query = jnp.einsum('btd,de->bte', normed.astype(jnp.float32), wq.astype(jnp.float32)).astype(jnp.bfloat16)
    keyvalue = jnp.einsum('bpd,de->bpe', memory.astype(jnp.float32), wkv_flat.astype(jnp.float32)).astype(jnp.bfloat16)
    keys = keyvalue[:, :, :inner].reshape(seqs, ENC_LEN, HEADS, HEAD_DIM)
    values = keyvalue[:, :, inner:].reshape(seqs, ENC_LEN, HEADS, HEAD_DIM)
    qh = query.reshape(seqs, DEC_LEN, HEADS, HEAD_DIM)
    scores = jnp.einsum('bqhd,bkhd->bhqk', qh.astype(jnp.float32), keys.astype(jnp.float32)) / jnp.sqrt(jnp.float32(HEAD_DIM))
    probs = jax.nn.softmax(scores, axis=-1).astype(jnp.bfloat16)
    context = jnp.einsum('bhqk,bkhd->bqhd', probs.astype(jnp.float32), values.astype(jnp.float32)).astype(jnp.bfloat16)
    context = context.reshape(seqs, DEC_LEN, inner)
    branch = jnp.einsum('bte,ed->btd', context.astype(jnp.float32), wo.astype(jnp.float32))
    return (xf + branch).astype(jnp.bfloat16)

def reference(memory, states, norm_gain, w_query, w_keyvalue, w_output):

    def run(packed):
        section_states, gain, wq, wkv, wo = packed
        return one_section(memory, section_states, gain, wq, wkv, wo)
    return lax.map(run, (states, norm_gain, w_query, w_keyvalue, w_output))
```

```python
import functools

import jax
import jax.numpy as jnp
from jax import lax
from jax.experimental import pallas as pl
from jax.experimental.pallas import tpu as pltpu
from jax.sharding import PartitionSpec as P

HEAD_DIM = 64
AXES = ("pipe", "tensor")


def device(x, y, z, c):
    x, y, z = x % 4, y % 4, z % 8
    return (y * 4 + z % 4) * 16 + x * 4 + (z // 4) * 2 + c


def send(value, route):
    pairs = [
        (device(x, y, z, c), device(*route(x, y, z, c)))
        for x in range(4)
        for y in range(4)
        for z in range(8)
        for c in range(2)
    ]
    return lax.ppermute(value, AXES, pairs)


def to_x(step):
    return lambda x, y, z, c: (x + step, y, z, c)


def to_partner_z(x, y, z, c):
    return x, y, z + 4, c


def to_core(x, y, z, c):
    return x, y, z, 1 - c


def split_x(x, y, z, c):
    return x + 1 - 2 * c, y, z, c


def split_y(x, y, z, c):
    return x, y + 1 - 2 * c, z, c


def split_z(step):
    return lambda x, y, z, c: (x, y, z + step * (1 - 2 * c), c)


VMEM = pl.BlockSpec(memory_space=pltpu.VMEM)


def call(body, shapes, args, flops, name):
    bytes_in = sum(a.size * a.dtype.itemsize for a in args)
    bytes_out = sum(s.size * s.dtype.itemsize for s in shapes)
    limit = min(60 << 20, int(1.1 * (bytes_in + bytes_out)) + (12 << 20))
    return pl.pallas_call(
        body,
        out_shape=shapes,
        in_specs=[VMEM] * len(args),
        out_specs=[VMEM] * len(shapes),
        compiler_params=pltpu.CompilerParams(vmem_limit_bytes=limit),
        cost_estimate=pl.CostEstimate(
            flops=flops, bytes_accessed=bytes_in + bytes_out, transcendentals=0
        ),
        name=name,
    )(*args)


def place():
    t, p = lax.axis_index("tensor"), lax.axis_index("pipe")
    return t // 4, (t // 2) % 2, t % 2, p % 4


def cat_body(counts, *refs):
    out, at = refs[-1], 0
    for ref, count in zip(refs[:-1], counts):
        out[at : at + count] = ref[...]
        at += count


def cat(*arrays):
    counts = [a.shape[0] for a in arrays]
    shape = jax.ShapeDtypeStruct((sum(counts),) + arrays[0].shape[1:], arrays[0].dtype)
    return call(functools.partial(cat_body, counts), [shape], arrays, 1 << 20, "cat")[0]


def kv_body(row_sets, *refs):
    w_ref, out_ref = refs[-2:]
    x, zhi, c, zlo = place()
    z = zhi * 4 + zlo + 8
    s = 1 - 2 * c
    flips = [
        0,
        zhi ^ (((z - s) % 8) // 4),
        zhi ^ (((z + s) % 8) // 4),
        zhi ^ (((z - 2 * s) % 8) // 4),
    ]
    flips.append(1 - flips[3])
    for at in range(0, len(row_sets), 4):
        group = row_sets[at : at + 4]
        total = None
        for rc in range(2):
            for rz in range(2):
                for k in range(4):
                    parts = []
                    for row_set in group:
                        piece, base, flip = row_set[rc]
                        parts.append(refs[piece][base + (rz ^ flips[flip]) * 4 + k])
                    f = ((x + k) % 4) * 4 + (zhi ^ rz) * 2 + (c ^ rc)
                    w = w_ref[pl.ds(pl.multiple_of(f * 256, 256), 256), :]
                    term = jnp.dot(
                        jnp.concatenate(parts, 0), w, preferred_element_type=jnp.float32
                    )
                    total = term if total is None else total + term
        out_ref[at : at + 4] = total.astype(jnp.bfloat16).reshape(4, 2, 32, 512)


def project(pieces, row_sets, w, name):
    n = len(row_sets)
    shape = jax.ShapeDtypeStruct((n, 2, 32, 512), jnp.bfloat16)
    flops = 2 * n * 64 * 4096 * 512
    return call(functools.partial(kv_body, row_sets), [shape], (*pieces, w), flops, name)[0]


def query_body(own, near, near_s, far, far_s, gain, w_ref, out_ref):
    x, zhi, c, _ = place()
    s = 1 - 2 * c
    blocks = []
    for ref, where, flip in ((own, x, 0), (near, x + 4 - s, 0), (near_s, x + s + 4, 1)):
        for rc in range(2):
            for rz in range(2):
                blocks.append((ref, rc * 2 + rz, where % 4, rz, rc ^ flip))
    for ref, flip in ((far, 0), (far_s, 1)):
        for rz in range(2):
            blocks.append((ref, rz, (x + 2) % 4, rz, flip))
    squares = None
    for ref, i, _, _, _ in blocks:
        v = ref[i].astype(jnp.float32)
        squares = v * v if squares is None else squares + v * v
    mean = jnp.sum(squares, axis=-1, keepdims=True) * (1.0 / 4096)
    scale = lax.rsqrt(mean + 1e-06)
    total = None
    for ref, i, where, rz, rc in blocks:
        f = where * 4 + (zhi ^ rz) * 2 + (c ^ rc)
        normed = (ref[i].astype(jnp.float32) * scale * gain[f]).astype(jnp.bfloat16)
        w = w_ref[pl.ds(pl.multiple_of(f * 256, 256), 256), :]
        term = jnp.dot(normed, w, preferred_element_type=jnp.float32)
        total = term if total is None else total + term
    out_ref[...] = total.astype(jnp.bfloat16)


def attend_body(b, q_ref, a_ref, b_ref, c_ref, out_ref):
    lane = lax.broadcasted_iota(jnp.int32, (256, 128), 1)

    def rows(lo):
        return jnp.concatenate(
            [r[:, b, :, lo : lo + 128].reshape(-1, 128) for r in (a_ref, b_ref, c_ref)], 0
        )

    for pair in range(2):
        q = q_ref[:, pair * 128 : pair * 128 + 128]
        keys, values = rows(pair * 128), rows(256 + pair * 128)
        outs = []
        for h in range(2):
            mine = lane // HEAD_DIM == h
            qh = jnp.where(mine, q, jnp.zeros_like(q))
            scores = lax.dot_general(
                qh, keys, (((1,), (1,)), ((), ())), preferred_element_type=jnp.float32
            )
            scores = scores * (1.0 / 8.0)
            e = jnp.exp(scores - jnp.max(scores, axis=-1, keepdims=True))
            probs = (e / jnp.sum(e, axis=-1, keepdims=True)).astype(jnp.bfloat16)
            outs.append(jnp.dot(probs, values, preferred_element_type=jnp.float32))
        out_ref[:, pair * 128 : pair * 128 + 128] = jnp.where(
            lane < HEAD_DIM, outs[0], outs[1]
        ).astype(jnp.bfloat16)


def output_body(ctx, ctx_s, w_ref, ws_ref, p0, p1, p2, p3):
    x, zhi, c, _ = place()
    for k, out in enumerate((p0, p1, p2, p3)):
        for j in range(2):
            f = ((x + k) % 4) * 4 + (zhi ^ j) * 2 + c
            cols = pl.ds(pl.multiple_of(f * 256, 256), 256)
            part = jnp.dot(ctx[...], w_ref[:, cols], preferred_element_type=jnp.float32)
            part += jnp.dot(ctx_s[...], ws_ref[:, cols], preferred_element_type=jnp.float32)
            out[:, j * 256 : j * 256 + 256] = part.astype(out.dtype)


def per_device(memory, states, norm_gain, w_query, w_keyvalue, w_output):
    mem = memory.reshape(64, 256)[None]
    w_kv = w_keyvalue[0].reshape(4096, 512)
    wo = w_output[0]
    st = [states[:, b] for b in range(2)]

    ahead = send(mem, to_x(-1))
    behind = send(mem, to_x(1))
    across = send(mem, to_x(2))
    st_z = [send(st[0], to_partner_z)]
    wo_s = send(wo, to_core)
    row = cat(mem, ahead, across, behind)
    row_z = send(row, to_partner_z)
    row_s = send(row, to_core)
    row_zs = send(row_z, to_core)
    block = cat(row, row_z, row_s, row_zs)

    near = send(block, split_z(1))
    far = send(block[:8], split_z(2))
    st_z.append(send(st[1], to_partner_z))
    near_s = send(near, to_core)
    far_s = send(far, to_core)
    far2 = cat(far, far_s)

    query = []
    for b in range(2):
        st_s = send(st[b], to_core)
        st_zs = send(st_z[b], to_core)
        own = cat(st[b], st_z[b], st_s, st_zs)
        s_near = send(own, split_x)
        s_near_s = send(s_near, to_core)
        s_far = send(s_near[:2], split_x)
        s_far_s = send(s_far, to_core)
        args = (own, s_near, s_near_s, s_far, s_far_s, norm_gain.reshape(16, 1, 256), w_query[0])
        shape = jax.ShapeDtypeStruct((256, 256), jnp.bfloat16)
        query.append(call(query_body, [shape], args, 2 * 256 * 4096 * 256, "query")[0])

    first, swapped, second, second_s = [], [], [], []
    for piece, late in ((block, False), (near, False), (near_s, True), (far2, False)):
        r1 = send(piece, split_y)
        r2 = send(r1[8:] if late else r1[:8], split_y)
        first.append(r1)
        swapped.append(send(r1, to_core))
        second.append(r2)
        second_s.append(send(r2, to_core))

    def plain(i, flip, far_flip=None):
        return ((i, 0, flip), (i, 8, flip if far_flip is None else far_flip))

    def crossed(i, flip, far_flip=None):
        return ((i, 8, flip), (i, 0, flip if far_flip is None else far_flip))

    sets_a = (plain(0, 0), plain(1, 1), crossed(2, 2), plain(3, 3, 4))
    sets_b = sets_a + (crossed(4, 0), crossed(5, 2), plain(6, 1), crossed(7, 3, 4))
    sets_c = (
        ((0, 0, 0), (4, 0, 0)),
        ((1, 0, 1), (6, 0, 1)),
        ((2, 0, 2), (5, 0, 2)),
        ((3, 0, 3), (7, 0, 4)),
    )
    kv_a = project((block, near, near_s, far2), sets_a, w_kv, "kv_a")
    kv_b = project((*first, *swapped), sets_b, w_kv, "kv_b")
    kv_c = project((*second, *second_s), sets_c, w_kv, "kv_c")

    outs = []
    for b in range(2):
        shape = jax.ShapeDtypeStruct((256, 256), jnp.bfloat16)
        args = (query[b], kv_a, kv_b, kv_c)
        ctx = call(functools.partial(attend_body, b), [shape], args, 1 << 30, "attend")[0]
        ctx_s = send(ctx, to_core)
        shapes = [jax.ShapeDtypeStruct((256, 512), jnp.float32)]
        shapes += [jax.ShapeDtypeStruct((256, 512), jnp.bfloat16)] * 3
        p0, p1, p2, p3 = call(output_body, shapes, (ctx, ctx_s, wo, wo_s), 1 << 30, "output")
        total = p0
        for part, step in ((p2, 2), (p1, 1), (p3, -1)):
            total = total + send(part, to_x(step)).astype(jnp.float32)
        away = send(total[:, 256:].astype(jnp.bfloat16), to_partner_z)
        out = states[0, b].astype(jnp.float32) + (total[:, :256] + away.astype(jnp.float32))
        outs.append(out.astype(jnp.bfloat16))
    return jnp.stack(outs)[None]


def solution(mesh):
    in_specs = (
        P(None, "pipe", "tensor"),
        P("pipe", None, None, "tensor"),
        P("pipe", None),
        P("pipe", None, "tensor"),
        P("pipe", None, None, "tensor"),
        P("pipe", "tensor", None),
    )
    out_specs = P("pipe", None, None, "tensor")
    return jax.shard_map(
        per_device, mesh=mesh, in_specs=in_specs, out_specs=out_specs, check_vma=False
    )
```

```python
import functools

import jax
import jax.numpy as jnp
from jax import lax
from jax.experimental import pallas as pl
from jax.experimental.pallas import tpu as pltpu
from jax.sharding import PartitionSpec as P


HEAD_DIM = 64
AXES = ("pipe", "tensor")


def device(x, y, z, c):
    x, y, z = x % 4, y % 4, z % 8
    return (y * 4 + z % 4) * 16 + x * 4 + (z // 4) * 2 + c


def send(value, route):
    pairs = [
        (device(x, y, z, c), device(*route(x, y, z, c)))
        for x in range(4)
        for y in range(4)
        for z in range(8)
        for c in range(2)
    ]
    return lax.ppermute(value, AXES, pairs)


def to_x(step):
    return lambda x, y, z, c: (x + step, y, z, c)


def to_partner_z(x, y, z, c):
    return x, y, z + 4, c


def to_core(x, y, z, c):
    return x, y, z, 1 - c


def split_x(x, y, z, c):
    return x + 1 - 2 * c, y, z, c


def split_y(x, y, z, c):
    return x, y + 1 - 2 * c, z, c


def split_z(x, y, z, c):
    return x, y, z + 1 - 2 * c, c


VMEM = pl.BlockSpec(memory_space=pltpu.VMEM)


def call(body, shapes, args, flops):
    bytes_in = sum(a.size * a.dtype.itemsize for a in args)
    bytes_out = sum(s.size * s.dtype.itemsize for s in shapes)
    limit = min(60 << 20, int(1.1 * (bytes_in + bytes_out)) + (12 << 20))
    return pl.pallas_call(
        body,
        out_shape=shapes,
        in_specs=[VMEM] * len(args),
        out_specs=[VMEM] * len(shapes),
        compiler_params=pltpu.CompilerParams(vmem_limit_bytes=limit),
        cost_estimate=pl.CostEstimate(
            flops=flops, bytes_accessed=bytes_in + bytes_out, transcendentals=0
        ),
    )(*args)


def place():
    t, p = lax.axis_index("tensor"), lax.axis_index("pipe")
    return t // 4, (t // 2) % 2, t % 2, p % 4


def cat_body(plan, *refs):
    out, at = refs[-1], 0
    for i, lo, count in plan:
        out[at : at + count] = refs[i][lo : lo + count]
        at += count


def cat(*parts):
    arrays, plan = [], []
    for part in parts:
        array, lo, count = part if isinstance(part, tuple) else (part, 0, part.shape[0])
        known = [i for i, a in enumerate(arrays) if a is array]
        if not known:
            known = [len(arrays)]
            arrays.append(array)
        plan.append((known[0], lo, count))
    rows = sum(count for _, _, count in plan)
    shape = jax.ShapeDtypeStruct((rows,) + arrays[0].shape[1:], arrays[0].dtype)
    return call(functools.partial(cat_body, plan), [shape], arrays, 1 << 20)[0]


def kv_body(row_sets, *refs):
    w_ref, out_ref = refs[-2:]
    x, zhi, c, zlo = place()
    z = zhi * 4 + zlo + 8
    s = 1 - 2 * c
    flips = [
        0,
        zhi ^ (((z - s) % 8) // 4),
        zhi ^ (((z + s) % 8) // 4),
        zhi ^ (((z - 2 * s) % 8) // 4),
    ]
    flips.append(1 - flips[3])
    for at in range(0, len(row_sets), 4):
        group = row_sets[at : at + 4]
        total = None
        for rc in range(2):
            for g in range(4):
                for rz in range(2):
                    parts = []
                    for row_set in group:
                        piece, base, flip = row_set[rc]
                        parts.append(refs[piece][base + g * 2 + (rz ^ flips[flip])])
                    f = ((x + g) % 4) * 4 + (zhi ^ rz) * 2 + (c ^ rc)
                    w = w_ref[pl.ds(pl.multiple_of(f * 256, 256), 256), :]
                    term = jnp.dot(
                        jnp.concatenate(parts, 0), w, preferred_element_type=jnp.float32
                    )
                    total = term if total is None else total + term
        out_ref[at : at + 4] = total.astype(jnp.bfloat16).reshape(4, 2, 32, 512)


def project(pieces, row_sets, w):
    n = len(row_sets)
    shape = jax.ShapeDtypeStruct((n, 2, 32, 512), jnp.bfloat16)
    flops = 2 * n * 64 * 4096 * 512
    body = functools.partial(kv_body, row_sets)
    return call(body, [shape], (*pieces, w), flops)[0]


def query_body(own, near, near_s, far, far_s, gain, w_ref, out_ref):
    x, zhi, c, _ = place()
    s = 1 - 2 * c
    blocks = []
    for ref, where, flip in ((own, x, 0), (near, x + 4 - s, 0), (near_s, x + s + 4, 1)):
        for rc in range(2):
            blocks.append((ref, rc * 2, where % 4, rc ^ flip))
    for ref, flip in ((far, 0), (far_s, 1)):
        blocks.append((ref, 0, (x + 2) % 4, flip))

    @pl.loop(0, 2)
    def _(half):
        rows = pl.ds(pl.multiple_of(half * 256, 256), 256)
        squares = None
        for ref, i, _, _ in blocks:
            for rz in range(2):
                v = ref[i + rz, rows].astype(jnp.float32)
                squares = v * v if squares is None else squares + v * v
        mean = jnp.sum(squares, axis=-1, keepdims=True) * (1.0 / 4096)
        scale = lax.rsqrt(mean + 1e-06)
        total = None
        for ref, i, where, rc in blocks:
            for rz in range(2):
                f = where * 4 + (zhi ^ rz) * 2 + (c ^ rc)
                v = ref[i + rz, rows].astype(jnp.float32)
                normed = (v * scale * gain[f]).astype(jnp.bfloat16)
                w = w_ref[pl.ds(pl.multiple_of(f * 256, 256), 256), :]
                term = jnp.dot(normed, w, preferred_element_type=jnp.float32)
                total = term if total is None else total + term
        out_ref[rows, :] = total.astype(jnp.bfloat16)


def attend_body(b, q_ref, a_ref, b_ref, c_ref, out_ref):
    lane = lax.broadcasted_iota(jnp.int32, (256, 128), 1)

    def rows(lo):
        return jnp.concatenate(
            [r[:, b, :, lo : lo + 128].reshape(-1, 128) for r in (a_ref, b_ref, c_ref)], 0
        )

    for pair in range(2):
        q = q_ref[b * 256 : b * 256 + 256, pair * 128 : pair * 128 + 128]
        keys, values = rows(pair * 128), rows(256 + pair * 128)
        outs = []
        for h in range(2):
            mine = lane // HEAD_DIM == h
            qh = jnp.where(mine, q, jnp.zeros_like(q))
            scores = lax.dot_general(
                qh, keys, (((1,), (1,)), ((), ())), preferred_element_type=jnp.float32
            )
            scores = scores * (1.0 / 8.0)
            e = jnp.exp(scores - jnp.max(scores, axis=-1, keepdims=True))
            probs = (e / jnp.sum(e, axis=-1, keepdims=True)).astype(jnp.bfloat16)
            outs.append(jnp.dot(probs, values, preferred_element_type=jnp.float32))
        out_ref[:, pair * 128 : pair * 128 + 128] = jnp.where(
            lane < HEAD_DIM, outs[0], outs[1]
        ).astype(jnp.bfloat16)


def output_body(side, refs_in, *refs):
    w_ref, ws_ref = refs[refs_in : refs_in + 2]
    x, zhi, c, _ = place()
    for k, out in enumerate(refs[refs_in + 2 :]):
        f = ((x + k) % 4) * 4 + (zhi ^ side) * 2 + c
        cols = pl.ds(pl.multiple_of(f * 256, 256), 256)
        for b in range(refs_in // 2):
            ctx, ctx_c = refs[2 * b : 2 * b + 2]
            part = jnp.dot(ctx[...], w_ref[:, cols], preferred_element_type=jnp.float32)
            part += jnp.dot(ctx_c[...], ws_ref[:, cols], preferred_element_type=jnp.float32)
            out[b * 256 : b * 256 + 256, :] = part.astype(out.dtype)


def products(side, contexts, w, w_c):
    rows = 128 * len(contexts)
    shapes = [jax.ShapeDtypeStruct((rows, 256), jnp.float32)]
    shapes += [jax.ShapeDtypeStruct((rows, 256), jnp.bfloat16)] * 3
    body = functools.partial(output_body, side, len(contexts))
    return call(body, shapes, (*contexts, w, w_c), 2 * rows * 512 * 1024)


def finish_body(st, own, far, up, down, away0, away1, out_ref):
    for b, away in enumerate((away0, away1)):
        rows = slice(b * 256, b * 256 + 256)
        total = own[rows, :]
        for part in (far, up, down):
            total = total + part[rows, :].astype(jnp.float32)
        total = total + away[...].astype(jnp.float32)
        out_ref[rows, :] = (st[0, rows].astype(jnp.float32) + total).astype(jnp.bfloat16)


def section(memory, states, norm_gain, w_query, w_keyvalue, w_output):
    mem = memory.reshape(1, 64, 256)
    st = states.reshape(1, 512, 256)
    w_kv = w_keyvalue[0].reshape(4096, 512)
    wo = w_output[0]

    mem_z = send(mem, to_partner_z)
    st_z = send(st, to_partner_z)
    pair = cat(cat(mem), mem_z)
    x_far = send(pair, to_x(2))
    x_up = send(pair, to_x(-1))
    x_down = send(pair, to_x(1))
    row = cat(pair, x_up, x_far, x_down)
    block = cat(row, send(row, to_core))

    near = send(block, split_z)
    far = send(near[:8], split_z)
    near_c = send(near, to_core)
    far_c = send(far, to_core)
    sides = cat(near_c, near)
    far2 = cat(far, far_c)

    st_pair = cat(cat(st), st_z)
    st_own = cat(st_pair, send(st_pair, to_core))
    s_near = send(st_own, split_x)
    s_near_c = send(s_near, to_core)
    s_far = send(s_near[:2], split_x)
    s_far_c = send(s_far, to_core)
    args = (st_own, s_near, s_near_c, s_far, s_far_c, norm_gain.reshape(16, 1, 256), w_query[0])
    shape = jax.ShapeDtypeStruct((512, 256), jnp.bfloat16)
    query = call(query_body, [shape], args, 2 * 512 * 4096 * 256)[0]

    first, swapped, second, second_c = [], [], [], []
    for i, piece in enumerate((block, sides, far2)):
        r1 = send(piece, split_y)
        r2 = send(r1[8:24] if i == 1 else r1[:8], split_y)
        first.append(r1)
        swapped.append(send(r1, to_core))
        second.append(r2)
        second_c.append(send(r2, to_core))

    def sets_of(i_block, i_sides, i_far):
        return (
            ((i_block, 0, 0), (i_block, 8, 0)),
            ((i_sides, 16, 1), (i_sides, 24, 1)),
            ((i_sides, 8, 2), (i_sides, 0, 2)),
            ((i_far, 0, 3), (i_far, 8, 4)),
        )

    sets_s = (
        ((3, 8, 0), (3, 0, 0)),
        ((4, 24, 2), (4, 16, 2)),
        ((4, 0, 1), (4, 8, 1)),
        ((5, 8, 3), (5, 0, 4)),
    )
    sets_c = (
        ((0, 0, 0), (3, 0, 0)),
        ((1, 8, 1), (4, 0, 1)),
        ((1, 0, 2), (4, 8, 2)),
        ((2, 0, 3), (5, 0, 4)),
    )
    kv_a = project((block, sides, far2), sets_of(0, 1, 2), w_kv)
    kv_b = project((*first, *swapped), sets_of(0, 1, 2) + sets_s, w_kv)
    kv_c = project((*second, *second_c), sets_c, w_kv)

    wo_c = send(wo, to_core)
    contexts, away = [], []
    for b in range(2):
        shape = jax.ShapeDtypeStruct((256, 256), jnp.bfloat16)
        args = (query, kv_a, kv_b, kv_c)
        ctx = call(functools.partial(attend_body, b), [shape], args, 1 << 30)[0]
        contexts += [ctx, send(ctx, to_core)]
        total, *parts = products(1, contexts[-2:], wo, wo_c)
        for part in scatter_x(parts):
            total = total + part.astype(jnp.float32)
        away.append(send(total.astype(jnp.bfloat16), to_partner_z))
    total, *parts = products(0, contexts, wo, wo_c)
    shape = jax.ShapeDtypeStruct((512, 256), jnp.bfloat16)
    args = (st, total, *scatter_x(parts), *away)
    out = call(finish_body, [shape], args, 1 << 20)[0]
    return out.reshape(states.shape)


def scatter_x(parts):
    next_x, far, previous = parts
    return (send(far, to_x(2)), send(next_x, to_x(1)), send(previous, to_x(-1)))


def solution(mesh):
    in_specs = (
        P(None, "pipe", "tensor"),
        P("pipe", None, None, "tensor"),
        P("pipe", None),
        P("pipe", None, "tensor"),
        P("pipe", None, None, "tensor"),
        P("pipe", "tensor", None),
    )
    out_specs = P("pipe", None, None, "tensor")
    return jax.shard_map(
        section, mesh=mesh, in_specs=in_specs, out_specs=out_specs, check_vma=False
    )
```

```python
import functools

import jax
import jax.numpy as jnp
from jax import lax
from jax.experimental import pallas as pl
from jax.experimental.pallas import tpu as pltpu
from jax.sharding import PartitionSpec as P


HEAD_DIM = 64
AXES = ("pipe", "tensor")


def device(x, y, z, c):
    x, y, z = x % 4, y % 4, z % 8
    return (y * 4 + z % 4) * 16 + x * 4 + (z // 4) * 2 + c


def send(value, route):
    pairs = [
        (device(x, y, z, c), device(*route(x, y, z, c)))
        for x in range(4)
        for y in range(4)
        for z in range(8)
        for c in range(2)
    ]
    return lax.ppermute(value, AXES, pairs)


def to_x(step):
    return lambda x, y, z, c: (x + step, y, z, c)


def to_partner_z(x, y, z, c):
    return x, y, z + 4, c


def to_core(x, y, z, c):
    return x, y, z, 1 - c


def split_x(x, y, z, c):
    return x + 1 - 2 * c, y, z, c


def split_y(x, y, z, c):
    return x, y + 1 - 2 * c, z, c


def split_z(x, y, z, c):
    return x, y, z + 1 - 2 * c, c


VMEM = pl.BlockSpec(memory_space=pltpu.VMEM)


def call(body, shapes, args, flops):
    bytes_in = sum(a.size * a.dtype.itemsize for a in args)
    bytes_out = sum(s.size * s.dtype.itemsize for s in shapes)
    limit = min(60 << 20, int(1.1 * (bytes_in + bytes_out)) + (12 << 20))
    return pl.pallas_call(
        body,
        out_shape=shapes,
        in_specs=[VMEM] * len(args),
        out_specs=[VMEM] * len(shapes),
        compiler_params=pltpu.CompilerParams(vmem_limit_bytes=limit),
        cost_estimate=pl.CostEstimate(
            flops=flops, bytes_accessed=bytes_in + bytes_out, transcendentals=0
        ),
    )(*args)


def place():
    t, p = lax.axis_index("tensor"), lax.axis_index("pipe")
    return t // 4, (t // 2) % 2, t % 2, p % 4


def cat_body(plan, *refs):
    out, at = refs[-1], 0
    for i, lo, count in plan:
        out[at : at + count] = refs[i][lo : lo + count]
        at += count


def cat(*parts):
    arrays, plan = [], []
    for part in parts:
        array, lo, count = part if isinstance(part, tuple) else (part, 0, part.shape[0])
        known = [i for i, a in enumerate(arrays) if a is array]
        if not known:
            known = [len(arrays)]
            arrays.append(array)
        plan.append((known[0], lo, count))
    rows = sum(count for _, _, count in plan)
    shape = jax.ShapeDtypeStruct((rows,) + arrays[0].shape[1:], arrays[0].dtype)
    return call(functools.partial(cat_body, plan), [shape], arrays, 1 << 20)[0]


def kv_body(row_sets, *refs):
    w_ref, out_ref = refs[-2:]
    x, zhi, c, zlo = place()
    z = zhi * 4 + zlo + 8
    s = 1 - 2 * c
    flips = [
        0,
        zhi ^ (((z - s) % 8) // 4),
        zhi ^ (((z + s) % 8) // 4),
        zhi ^ (((z - 2 * s) % 8) // 4),
    ]
    flips.append(1 - flips[3])
    step = 3 if len(row_sets) % 3 == 0 else 4
    for at in range(0, len(row_sets), step):
        group = row_sets[at : at + step]
        total = None
        for rc in range(2):
            for g in range(4):
                for rz in range(2):
                    parts = []
                    for row_set in group:
                        piece, base, flip = row_set[rc]
                        parts.append(refs[piece][base + g * 2 + (rz ^ flips[flip])])
                    f = ((x + g) % 4) * 4 + (zhi ^ rz) * 2 + (c ^ rc)
                    w = w_ref[pl.ds(pl.multiple_of(f * 256, 256), 256), :]
                    term = jnp.dot(
                        jnp.concatenate(parts, 0), w, preferred_element_type=jnp.float32
                    )
                    total = term if total is None else total + term
        n = len(group)
        out_ref[at : at + n] = total.astype(jnp.bfloat16).reshape(n, 2, 32, 512)


def project(pieces, row_sets, w):
    n = len(row_sets)
    shape = jax.ShapeDtypeStruct((n, 2, 32, 512), jnp.bfloat16)
    flops = 2 * n * 64 * 4096 * 512
    body = functools.partial(kv_body, row_sets)
    return call(body, [shape], (*pieces, w), flops)[0]


def query_body(own, near, near_s, far, far_s, gain, w_ref, out_ref):
    x, zhi, c, _ = place()
    s = 1 - 2 * c
    blocks = []
    for ref, where, flip in ((own, x, 0), (near, x + 4 - s, 0), (near_s, x + s + 4, 1)):
        for rc in range(2):
            blocks.append((ref, rc * 2, where % 4, rc ^ flip))
    for ref, flip in ((far, 0), (far_s, 1)):
        blocks.append((ref, 0, (x + 2) % 4, flip))

    @pl.loop(0, 2)
    def _(half):
        rows = pl.ds(pl.multiple_of(half * 256, 256), 256)
        squares = None
        for ref, i, _, _ in blocks:
            for rz in range(2):
                v = ref[i + rz, rows].astype(jnp.float32)
                squares = v * v if squares is None else squares + v * v
        mean = jnp.sum(squares, axis=-1, keepdims=True) * (1.0 / 4096)
        scale = lax.rsqrt(mean + 1e-06)
        total = None
        for ref, i, where, rc in blocks:
            for rz in range(2):
                f = where * 4 + (zhi ^ rz) * 2 + (c ^ rc)
                v = ref[i + rz, rows].astype(jnp.float32)
                normed = (v * scale * gain[f]).astype(jnp.bfloat16)
                w = w_ref[pl.ds(pl.multiple_of(f * 256, 256), 256), :]
                term = jnp.dot(normed, w, preferred_element_type=jnp.float32)
                total = term if total is None else total + term
        out_ref[rows, :] = total.astype(jnp.bfloat16)


def attend_body(b, q_ref, a_ref, b_ref, c_ref, out_ref):
    lane = lax.broadcasted_iota(jnp.int32, (256, 128), 1)

    def rows(lo):
        return jnp.concatenate(
            [r[:, b, :, lo : lo + 128].reshape(-1, 128) for r in (a_ref, b_ref, c_ref)], 0
        )

    for pair in range(2):
        q = q_ref[b * 256 : b * 256 + 256, pair * 128 : pair * 128 + 128]
        keys, values = rows(pair * 128), rows(256 + pair * 128)
        outs = []
        for h in range(2):
            mine = lane // HEAD_DIM == h
            qh = jnp.where(mine, q, jnp.zeros_like(q))
            scores = lax.dot_general(
                qh, keys, (((1,), (1,)), ((), ())), preferred_element_type=jnp.float32
            )
            scores = scores * (1.0 / 8.0)
            e = jnp.exp(scores - jnp.max(scores, axis=-1, keepdims=True))
            probs = (e * (1.0 / jnp.sum(e, axis=-1, keepdims=True))).astype(jnp.bfloat16)
            outs.append(jnp.dot(probs, values, preferred_element_type=jnp.float32))
        out_ref[:, pair * 128 : pair * 128 + 128] = jnp.where(
            lane < HEAD_DIM, outs[0], outs[1]
        ).astype(jnp.bfloat16)


def output_body(side, refs_in, *refs):
    w_ref, ws_ref = refs[refs_in : refs_in + 2]
    x, zhi, c, _ = place()
    for k, out in enumerate(refs[refs_in + 2 :]):
        f = ((x + k) % 4) * 4 + (zhi ^ side) * 2 + c
        cols = pl.ds(pl.multiple_of(f * 256, 256), 256)
        for b in range(refs_in // 2):
            ctx, ctx_c = refs[2 * b : 2 * b + 2]
            part = jnp.dot(ctx[...], w_ref[:, cols], preferred_element_type=jnp.float32)
            part += jnp.dot(ctx_c[...], ws_ref[:, cols], preferred_element_type=jnp.float32)
            out[b * 256 : b * 256 + 256, :] = part.astype(out.dtype)


def products(side, contexts, w, w_c):
    rows = 128 * len(contexts)
    shapes = [jax.ShapeDtypeStruct((rows, 256), jnp.float32)]
    shapes += [jax.ShapeDtypeStruct((rows, 256), jnp.bfloat16)] * 3
    body = functools.partial(output_body, side, len(contexts))
    return call(body, shapes, (*contexts, w, w_c), 2 * rows * 512 * 1024)


def finish_body(st, own, far, up, down, away0, away1, out_ref):
    for b, away in enumerate((away0, away1)):
        rows = slice(b * 256, b * 256 + 256)
        total = own[rows, :]
        for part in (far, up, down):
            total = total + part[rows, :].astype(jnp.float32)
        total = total + away[...].astype(jnp.float32)
        out_ref[rows, :] = (st[0, rows].astype(jnp.float32) + total).astype(jnp.bfloat16)


def section(memory, states, norm_gain, w_query, w_keyvalue, w_output):
    mem = memory.reshape(1, 64, 256)
    st = states.reshape(1, 512, 256)
    w_kv = w_keyvalue[0].reshape(4096, 512)
    wo = w_output[0]

    mem_z = send(mem, to_partner_z)
    st_z = send(st, to_partner_z)
    pair = cat(cat(mem), mem_z)
    x_far = send(pair, to_x(2))
    x_up = send(pair, to_x(-1))
    x_down = send(pair, to_x(1))
    row = cat(pair, x_up, x_far, x_down)
    block = cat(row, send(row, to_core))

    near = send(block, split_z)
    far = send(near[:8], split_z)
    near_c = send(near, to_core)
    far_c = send(far, to_core)
    sides = cat(near_c, near)
    far2 = cat(far, far_c)

    st_pair = cat(cat(st), st_z)
    st_own = cat(st_pair, send(st_pair, to_core))
    s_near = send(st_own, split_x)
    s_near_c = send(s_near, to_core)
    s_far = send(s_near[:2], split_x)
    s_far_c = send(s_far, to_core)
    args = (st_own, s_near, s_near_c, s_far, s_far_c, norm_gain.reshape(16, 1, 256), w_query[0])
    shape = jax.ShapeDtypeStruct((512, 256), jnp.bfloat16)
    query = call(query_body, [shape], args, 2 * 512 * 4096 * 256)[0]

    first, swapped, second, second_c = [], [], [], []
    for i, piece in enumerate((block, sides, far2)):
        r1 = send(piece, split_y)
        r2 = send(r1[8:24] if i == 1 else r1[:8], split_y)
        first.append(r1)
        swapped.append(send(r1, to_core))
        second.append(r2)
        second_c.append(send(r2, to_core))

    def sets_of(i_block, i_sides, i_far):
        return (
            ((i_block, 0, 0), (i_block, 8, 0)),
            ((i_sides, 16, 1), (i_sides, 24, 1)),
            ((i_sides, 8, 2), (i_sides, 0, 2)),
            ((i_far, 0, 3), (i_far, 8, 4)),
        )

    sets_a = sets_of(0, 1, 2) + (
        ((3, 0, 0), (3, 8, 0)),
        ((4, 8, 0), (4, 0, 0)),
        ((5, 0, 0), (6, 0, 0)),
    )
    sets_b = (
        ((0, 16, 1), (0, 24, 1)),
        ((0, 8, 2), (0, 0, 2)),
        ((1, 24, 2), (1, 16, 2)),
        ((1, 0, 1), (1, 8, 1)),
        ((2, 0, 3), (2, 8, 4)),
        ((3, 8, 3), (3, 0, 4)),
    )
    sets_c = (
        ((0, 8, 1), (1, 0, 1)),
        ((0, 0, 2), (1, 8, 2)),
        ((2, 0, 3), (3, 0, 4)),
    )
    early = (block, sides, far2, first[0], swapped[0], second[0], second_c[0])
    kv_a = project(early, sets_a, w_kv)
    kv_b = project((first[1], swapped[1], first[2], swapped[2]), sets_b, w_kv)
    kv_c = project((second[1], second_c[1], second[2], second_c[2]), sets_c, w_kv)

    wo_c = send(wo, to_core)
    contexts, away = [], []
    for b in range(2):
        shape = jax.ShapeDtypeStruct((256, 256), jnp.bfloat16)
        args = (query, kv_a, kv_b, kv_c)
        ctx = call(functools.partial(attend_body, b), [shape], args, 1 << 30)[0]
        contexts += [ctx, send(ctx, to_core)]
        total, *parts = products(1, contexts[-2:], wo, wo_c)
        for part in scatter_x(parts):
            total = total + part.astype(jnp.float32)
        away.append(send(total.astype(jnp.bfloat16), to_partner_z))
    total, *parts = products(0, contexts, wo, wo_c)
    shape = jax.ShapeDtypeStruct((512, 256), jnp.bfloat16)
    args = (st, total, *scatter_x(parts), *away)
    out = call(finish_body, [shape], args, 1 << 20)[0]
    return out.reshape(states.shape)


def scatter_x(parts):
    next_x, far, previous = parts
    return (send(far, to_x(2)), send(next_x, to_x(1)), send(previous, to_x(-1)))


def solution(mesh):
    in_specs = (
        P(None, "pipe", "tensor"),
        P("pipe", None, None, "tensor"),
        P("pipe", None),
        P("pipe", None, "tensor"),
        P("pipe", None, None, "tensor"),
        P("pipe", "tensor", None),
    )
    out_specs = P("pipe", None, None, "tensor")
    return jax.shard_map(
        section, mesh=mesh, in_specs=in_specs, out_specs=out_specs, check_vma=False
    )
```
